256 devices in a mesh: leaf: 64 (over x, z, core), rhs: 4 (over y).
Axes of the slice: x: 4, y: 4, z: 8, core: 2. Of those that a mesh axis runs over, the one named last changes fastest.
Arguments:
- coords: bfloat16 [64, 262144], P(None, 'leaf'), may hold values from -1.5 to 1.5
- rhs: bfloat16 [256, 262144], P('rhs', 'leaf'), parts along dimension 0, may hold values from -6 to 6
- basis: bfloat16 [512, 512, 256], P('leaf'), may hold values from -0.25 to 0.25
- transfer_one: bfloat16 [256, 512, 256], P('leaf'), may hold values from -0.25 to 0.25
- transfer_two: bfloat16 [128, 512, 256], P('leaf'), may hold values from -0.25 to 0.25
- far_blocks: bfloat16 [896, 4, 256, 256], P('leaf'), may hold values from -0.375 to 0.375
- neighbours: int32 [512, 8], replicated, may hold values from 0 to 511, as said below
- far_lists: int32 [896, 4], replicated, may hold values from 0 to 895, as said below
Outputs:
- product: float32 [256, 262144], P('rhs', 'leaf'), parts along dimension 0
The draws below stay inside these ranges and needn't reach their ends.
There are 4 independent parts, one for each index of `rhs`. The reference program is written for one: setup_inputs(seed, part) draws one part's arguments, and reference() takes and returns one part's arrays. A program takes and returns all parts, laid end to end along the dimension named above; an argument that names none is the same for every part. Nothing has to cross between parts.
Inputs may be any that keep to these rules, and one draw needn't show every extreme that they name: `neighbours`: row i starts with leaf i itself; its other entries name leaves of other devices (leaf i lies on device i // 8). The entries after the first in the lists of one device's leaves name no other device more than 1 times, and the leaves of every device are named exactly 56 times by such entries over all lists. `far_lists`: entry (n, f) names a node of the same level as node n on another device (node n lies on device n // 14). The entries of one device's nodes name no other device more than 1 times, and the nodes of every device are named exactly 56 times over all entries.
All inputs are finite; a program needn't handle non-finite values.
Results may differ from the reference program's by a relative error of at most 0.005.
Values may be sent and summed in bfloat16 or wider, within the bound.
No kernel may reach another device: no remote copies, remote signals or barrier semaphores. Data moves between devices by JAX's collectives and lax.ppermute only.
A program may use at most 128 MiB of HBM per device.

```python
import jax
import jax.numpy as jnp
from jax import lax

FEAT = 64
RANK = 256
R = 64
LEAF = 512
NB = 8
FAR = 4
LEAF_DEV = 8
LEAVES = 512
POINTS = 262144
NODE_DEV = 14
NODES = 896
N_LEAF = 64


def peer_targets(key, entry_count, peer_count):
    first_key, second_key = jax.random.split(key)
    placing = jax.random.permutation(first_key, peer_count).astype(jnp.int32)
    inverse = jnp.argsort(placing).astype(jnp.int32)
    offsets = (jax.random.permutation(second_key, peer_count - 1) + 1).astype(jnp.int32)
    chosen = offsets[jnp.arange(entry_count, dtype=jnp.int32) % (peer_count - 1)]
    devices = jnp.arange(peer_count, dtype=jnp.int32)
    return placing[(inverse[devices][:, None] + chosen[None, :]) % peer_count]


def draw_neighbours(key, part):
    peer_count = LEAVES // LEAF_DEV
    entry_count = (NB - 1) * LEAF_DEV
    first_key, second_key = jax.random.split(jax.random.fold_in(key, 11))
    owners = peer_targets(first_key, entry_count, peer_count)
    picked = jax.random.randint(second_key, (peer_count, entry_count), 0, LEAF_DEV, dtype=jnp.int32)
    remote = (owners * LEAF_DEV + picked).reshape(LEAVES, NB - 1)
    itself = jnp.arange(LEAVES, dtype=jnp.int32)[:, None]
    return jnp.concatenate([itself, remote], axis=1).astype(jnp.int32)


def draw_far_lists(key, part):
    peer_count = LEAVES // LEAF_DEV
    entry_count = NODE_DEV * FAR
    first_key, second_key = jax.random.split(jax.random.fold_in(key, 23))
    owners = peer_targets(first_key, entry_count, peer_count)
    asking = jnp.arange(entry_count, dtype=jnp.int32) // FAR
    level_start = jnp.where(asking < LEAF_DEV, 0, jnp.where(asking < LEAF_DEV * 3 // 2, LEAF_DEV, LEAF_DEV * 3 // 2))
    level_width = jnp.where(asking < LEAF_DEV, LEAF_DEV, jnp.where(asking < LEAF_DEV * 3 // 2, LEAF_DEV // 2, LEAF_DEV // 4))
    raw_pick = jax.random.randint(second_key, (peer_count, entry_count), 0, 1 << 20, dtype=jnp.int32)
    remote = owners * NODE_DEV + level_start[None, :] + raw_pick % level_width[None, :]
    return remote.reshape(NODES, FAR).astype(jnp.int32)


def level_of(own_key, dims, cuts, least, largest):
    level, own = 1.0, jax.random.fold_in(own_key, 6)
    for position, shards_of in cuts:
        draws = jnp.exp(jax.random.uniform(jax.random.fold_in(own, position), (shards_of,), jnp.float32, least / len(cuts), largest / len(cuts)))
        level = level * jnp.repeat(draws, dims[position] // shards_of).reshape([-1 if axis == position else 1 for axis in range(len(dims))])
    return level


def noise(stream_key, dims, scale, limit, cuts=(), kind=jnp.bfloat16):
    values = scale * jax.random.normal(stream_key, dims, jnp.float32)
    if cuts:
        values = values * level_of(stream_key, dims, cuts, -0.22, 0.18)
    return jnp.clip(values, -limit, limit).astype(kind)


def setup_inputs(seed: int = 0, part: int = 0) -> dict:
    splits = jax.random.split(jax.random.key(seed), 9)
    own_keys = jax.random.split(jax.random.fold_in(splits[8], part), 9)
    return {
        "coords": noise(splits[0], (FEAT, POINTS), 0.25, 1.5, ((1, 64),)),
        "rhs": noise(own_keys[1], (R, POINTS), 1.0, 6.0, ((1, 64),)),
        "basis": noise(splits[2], (LEAVES, LEAF, RANK), LEAF ** -0.5, 0.25, ((0, 64),)),
        "transfer_one": noise(splits[3], (LEAVES // 2, 2 * RANK, RANK), (2 * RANK) ** -0.5, 0.25, ((0, 64),)),
        "transfer_two": noise(splits[4], (LEAVES // 4, 2 * RANK, RANK), (2 * RANK) ** -0.5, 0.25, ((0, 64),)),
        "far_blocks": noise(splits[5], (NODES, FAR, RANK, RANK), RANK ** -0.5, 0.375, ((0, 64),)),
        "neighbours": draw_neighbours(jax.random.fold_in(splits[8], 71), part),
        "far_lists": draw_far_lists(jax.random.fold_in(splits[8], 71), part),
    }


def round_half(values):
    return lax.optimization_barrier(values.astype(jnp.bfloat16))


def kernel_tiles(sources, targets):
    src_f = sources.astype(jnp.float32)
    dst_f = targets.astype(jnp.float32)
    inner = jnp.einsum("...fa,...fb->...ab", src_f, dst_f, precision=lax.Precision.HIGHEST)
    src_sq = jnp.sum(src_f * src_f, axis=-2)
    dst_sq = jnp.sum(dst_f * dst_f, axis=-2)
    return round_half(jnp.exp(inner - 0.5 * src_sq[..., :, None] - 0.5 * dst_sq[..., None, :]))


def join_pairs(skeleton):
    return skeleton.reshape(-1, 2, R, RANK).transpose(0, 2, 1, 3).reshape(-1, R, 2 * RANK)


def descend(parent, transfer, child_far):
    rounded = round_half(parent).astype(jnp.float32)
    spread = jnp.einsum("mrk,mjk->mrj", rounded, transfer.astype(jnp.float32), precision=lax.Precision.HIGHEST)
    spread = spread.reshape(-1, R, 2, RANK).transpose(0, 2, 1, 3).reshape(-1, R, RANK)
    return child_far + spread


def reference(coords, rhs, basis, transfer_one, transfer_two, far_blocks, neighbours, far_lists):
    points = coords.reshape(FEAT, LEAVES, LEAF).transpose(1, 0, 2)
    charges = rhs.reshape(R, LEAVES, LEAF).transpose(1, 0, 2)

    def near_leaf(index):
        listed = neighbours[index]
        kernel = kernel_tiles(points[listed], points[index][None])
        return jnp.einsum("nra,nab->rb", charges[listed].astype(jnp.float32), kernel.astype(jnp.float32), precision=lax.Precision.HIGHEST)

    near = lax.map(near_leaf, jnp.arange(LEAVES, dtype=jnp.int32))
    skel_zero = round_half(jnp.einsum("lra,lak->lrk", charges.astype(jnp.float32), basis.astype(jnp.float32), precision=lax.Precision.HIGHEST))
    skel_one = round_half(jnp.einsum("mrj,mjk->mrk", join_pairs(skel_zero).astype(jnp.float32), transfer_one.astype(jnp.float32), precision=lax.Precision.HIGHEST))
    skel_two = round_half(jnp.einsum("mrj,mjk->mrk", join_pairs(skel_one).astype(jnp.float32), transfer_two.astype(jnp.float32), precision=lax.Precision.HIGHEST))
    skeleton = jnp.concatenate([
        skel_zero.reshape(N_LEAF, LEAF_DEV, R, RANK),
        skel_one.reshape(N_LEAF, LEAF_DEV // 2, R, RANK),
        skel_two.reshape(N_LEAF, LEAF_DEV // 4, R, RANK)], axis=1).reshape(NODES, R, RANK)
    far = jnp.zeros((NODES, R, RANK), jnp.float32)
    for partner in range(FAR):
        weights = skeleton[far_lists[:, partner]].astype(jnp.float32)
        far = far + jnp.einsum("nrk,nkj->nrj", weights, far_blocks[:, partner].astype(jnp.float32), precision=lax.Precision.HIGHEST)
    far = far.reshape(N_LEAF, NODE_DEV, R, RANK)
    far_zero = far[:, :LEAF_DEV].reshape(LEAVES, R, RANK)
    far_one = far[:, LEAF_DEV:LEAF_DEV * 3 // 2].reshape(LEAVES // 2, R, RANK)
    far_two = far[:, LEAF_DEV * 3 // 2:].reshape(LEAVES // 4, R, RANK)
    middle = descend(far_two, transfer_two, far_one)
    lowest = descend(middle, transfer_one, far_zero)
    lowest_rounded = round_half(lowest).astype(jnp.float32)
    result = near + jnp.einsum("lrk,lak->lra", lowest_rounded, basis.astype(jnp.float32), precision=lax.Precision.HIGHEST)
    return result.transpose(1, 0, 2).reshape(R, POINTS)
```

```python
import functools

import jax
import jax.numpy as jnp
from jax import lax
from jax.experimental import pallas as pl
from jax.experimental.pallas import tpu as pltpu
from jax.sharding import PartitionSpec as P


FEAT = 64
RANK = 256
R = 64
LEAF = 512
NB = 8
FAR = 4
NX, NZ, NC, NY = 4, 8, 2, 4
GROUP = NX * NC
LEAF_DEV = 8
NODE_DEV = 14
QUART = FEAT // NY
ROWS = R + QUART
AUG = 128
OFFSETS = (0, -1, 1, -2, 2, -3, 3, 4)
LEAF_CHUNKS = (((0, 3), (3, 5)), ((5, 7),), ((7, 8),))
NODE_CHUNKS = ((0, 5), (5, 8))


F32 = jnp.float32
BF16 = jnp.bfloat16


def place(x, z, c):
    return (x * NZ + z % NZ) * NC + c


def ring(step):
    return [
        (place(x, z, c), place(x, z + step, c))
        for x in range(NX)
        for z in range(NZ)
        for c in range(NC)
    ]


ROW_GROUPS = [[place(x, z, c) for x in range(NX) for c in range(NC)] for z in range(NZ)]


def cost(micros):
    return pl.CostEstimate(flops=int(micros * 1e9), bytes_accessed=0, transcendentals=0)


VMEM = pl.BlockSpec(memory_space=pltpu.VMEM)
SMEM = pl.BlockSpec(memory_space=pltpu.SMEM)


def call(kernel, micros, out, tables, arrays, scratch=(), megabytes=16):
    return pl.pallas_call(
        kernel,
        in_specs=[SMEM] * len(tables) + [VMEM] * len(arrays),
        out_specs=jax.tree.map(lambda _: VMEM, out),
        out_shape=out,
        scratch_shapes=list(scratch),
        compiler_params=pltpu.CompilerParams(vmem_limit_bytes=megabytes << 20),
        cost_estimate=cost(micros),
    )(*tables, *arrays)


def shaped(shape, kind):
    return jax.ShapeDtypeStruct(shape, kind)


def nt(a, b):
    return lax.dot_general(a, b, (((1,), (1,)), ((), ())), preferred_element_type=F32)


def pack_kernel(y_ref, rhs_ref, coords_ref, out_ref):
    start = pl.multiple_of(y_ref[0] * QUART, QUART)
    for leaf in range(LEAF_DEV):
        columns = slice(leaf * LEAF, (leaf + 1) * LEAF)
        out_ref[leaf, :R, :] = rhs_ref[:, columns]
        out_ref[leaf, R:, :] = coords_ref[pl.ds(start, QUART), columns]


def pack(y, rhs, coords):
    out = shaped((LEAF_DEV, ROWS, LEAF), BF16)
    return call(pack_kernel, 1, out, (y,), (rhs, coords), megabytes=8)


def square_rows(pieces, source):
    total = None
    for piece in pieces:
        wide = piece.astype(F32)
        part = jnp.sum(wide * wide, axis=0, keepdims=True)
        total = part if total is None else total + part
    total = total * -0.5
    high = total.astype(BF16).astype(F32)
    rest = total - high
    middle = rest.astype(BF16).astype(F32)
    low = rest - middle
    row = lax.broadcasted_iota(jnp.int32, (16, LEAF), 0)
    own = row if source else row - 3
    other = row - 3 if source else row
    block = jnp.where(own == 0, high, jnp.where(own == 1, middle, jnp.where(own == 2, low, 0.0)))
    block = jnp.where(jnp.logical_and(other >= 0, other < 3), 1.0, block)
    return block.astype(BF16)


def tile_product(target, spread, charges):
    exponent = jnp.dot(target, spread, preferred_element_type=F32)
    return nt(jnp.exp(exponent).astype(BF16), charges)


def own_kernel(y_ref, rhs_ref, coords_ref, target_ref, near_ref, spread_ref):
    y = y_ref[0]
    empty = jnp.zeros((AUG - FEAT - 16, LEAF), BF16)
    for leaf in range(LEAF_DEV):
        columns = slice(leaf * LEAF, (leaf + 1) * LEAF)
        pieces = []
        for shift in (0, NY - 1, 1, 2):
            start = pl.multiple_of(lax.rem(y + shift, NY) * QUART, QUART)
            pieces.append(coords_ref[pl.ds(start, QUART), columns])
        wide = jnp.concatenate(pieces + [square_rows(pieces, False), empty], axis=0)
        target_ref[leaf] = wide.astype(F32).T.astype(BF16)
        spread_ref[leaf, :FEAT, :] = jnp.concatenate(pieces, axis=0)
        spread_ref[leaf, FEAT : FEAT + 16, :] = square_rows(pieces, True)
        spread_ref[leaf, FEAT + 16 :, :] = empty

    def pair(i, carry):
        for leaf in (2 * i, 2 * i + 1):
            charges = rhs_ref[:, pl.ds(pl.multiple_of(leaf * LEAF, LEAF), LEAF)]
            near_ref[leaf] = tile_product(target_ref[leaf], spread_ref[leaf], charges)
        return carry

    lax.fori_loop(0, LEAF_DEV // 2, pair, 0)


def own_tiles(y, rhs, coords):
    out = [shaped((LEAF_DEV, LEAF, AUG), BF16), shaped((LEAF_DEV, LEAF, R), F32)]
    scratch = [pltpu.VMEM((LEAF_DEV, AUG, LEAF), BF16)]
    return call(own_kernel, 5, out, (y,), (rhs, coords), scratch)


UNROLL = 4


def near_kernel(chunks, take_ref, *refs):
    got_refs = refs[: len(chunks)]
    a_ref, b_ref, c_ref, target_ref, before_ref, near_ref, spread_ref = refs[len(chunks) :]
    near_ref[...] = before_ref[...]
    spread_ref[:, FEAT + 16 :, :] = jnp.zeros((UNROLL, AUG - FEAT - 16, LEAF), BF16)
    start = chunks[0][0]
    for (low, high), got_ref in zip(chunks, got_refs, strict=True):
        count = high - low

        def some(i, carry, low=low, count=count, got_ref=got_ref):
            for buffer in range(UNROLL):
                item = i * UNROLL + buffer
                source, slot = item // count, item % count
                which = take_ref[source, low + slot]
                place_of = low - start + slot
                pieces = [got_ref[source, slot, R:, :]]
                pieces += [ref[source, place_of] for ref in (a_ref, b_ref, c_ref)]
                for q, piece in enumerate(pieces):
                    spread_ref[buffer, q * QUART : (q + 1) * QUART, :] = piece
                spread_ref[buffer, FEAT : FEAT + 16, :] = square_rows(pieces, True)
                charges = got_ref[source, slot, :R, :]
                charges = jnp.where(which >= 0, charges, jnp.zeros_like(charges))
                leaf = jnp.maximum(which, 0)
                near_ref[leaf] += tile_product(target_ref[leaf], spread_ref[buffer], charges)
            return carry

        lax.fori_loop(0, GROUP * count // UNROLL, some, 0)


def near_chunk(chunks, take, got, others, targets, before):
    slots = sum(high - low for low, high in chunks)
    return call(
        functools.partial(near_kernel, chunks),
        3.2 * slots,
        shaped((LEAF_DEV, LEAF, R), F32),
        (take,),
        (*got, *others, targets, before),
        [pltpu.VMEM((UNROLL, AUG, LEAF), BF16)],
        32,
    )


def choose_kernel(first, halves, send_ref, *refs):
    out_ref = refs[-1]
    at = 0
    for slot, parts in enumerate(halves):
        for target in range(GROUP):
            item = send_ref[target, first + slot]
            size = refs[at].shape[0]
            block = refs[at][jnp.minimum(item, size - 1)]
            if parts == 2:
                block = jnp.where(item >= size, refs[at + 1][jnp.maximum(item - size, 0)], block)
            out_ref[target, slot] = block
        at += parts


def choose(first, send, sources):
    halves = tuple(len(s) for s in sources)
    shape = sources[0][0].shape[1:]
    out = shaped((GROUP, len(sources), *shape), BF16)
    arrays = [array for parts in sources for array in parts]
    kernel = functools.partial(choose_kernel, first, halves)
    return call(kernel, 1, out, (send,), arrays)


def skeleton_kernel(leaves_ref, basis_ref, one_ref, two_ref, out_ref):
    def rounded_dot(a, b):
        return jnp.dot(a, b, preferred_element_type=F32).astype(BF16)

    for leaf in range(LEAF_DEV):
        out_ref[leaf] = rounded_dot(leaves_ref[leaf, :R, :], basis_ref[leaf])
    for m in range(LEAF_DEV // 2):
        joined = jnp.concatenate([out_ref[2 * m], out_ref[2 * m + 1]], axis=1)
        out_ref[LEAF_DEV + m] = rounded_dot(joined, one_ref[m])
    for m in range(LEAF_DEV // 4):
        low = LEAF_DEV + 2 * m
        joined = jnp.concatenate([out_ref[low], out_ref[low + 1]], axis=1)
        out_ref[LEAF_DEV * 3 // 2 + m] = rounded_dot(joined, two_ref[m])


def skeletons(leaves, basis, one, two):
    out = shaped((NODE_DEV, R, RANK), BF16)
    return call(skeleton_kernel, 3, out, (), (leaves, basis, one, two))


def far_kernel(low, high, fresh, take_ref, got_ref, blocks_ref, *refs):
    out_ref = refs[-1]
    out_ref[...] = jnp.zeros_like(out_ref) if fresh else refs[0][...]
    count = high - low

    def source_of(source, carry):
        for slot in range(count):
            which = take_ref[source, low + slot]
            weights = got_ref[source, slot]
            weights = jnp.where(which >= 0, weights, jnp.zeros_like(weights))
            at = jnp.maximum(which, 0)
            out_ref[at // FAR] += jnp.dot(
                weights, blocks_ref[at], preferred_element_type=F32
            )
        return carry

    lax.fori_loop(0, GROUP, source_of, 0)


def far_chunk(low, high, take, got, blocks, before):
    fresh = before is None
    return call(
        functools.partial(far_kernel, low, high, fresh),
        high - low,
        shaped((NODE_DEV, R, RANK), F32),
        (take,),
        (got, blocks) + (() if fresh else (before,)),
    )


def finish_kernel(far_ref, one_ref, two_ref, basis_ref, near_ref, out_ref):
    for m in range(LEAF_DEV // 4):
        spread = nt(far_ref[LEAF_DEV * 3 // 2 + m].astype(BF16), two_ref[m])
        for side in range(2):
            node = 2 * m + side
            middle = far_ref[LEAF_DEV + node] + spread[:, side * RANK : (side + 1) * RANK]
            lower = nt(middle.astype(BF16), one_ref[node])
            for part in range(2):
                leaf = 2 * node + part
                lowest = far_ref[leaf] + lower[:, part * RANK : (part + 1) * RANK]
                columns = slice(leaf * LEAF, (leaf + 1) * LEAF)
                out_ref[:, columns] = near_ref[leaf].T + nt(lowest.astype(BF16), basis_ref[leaf])


def finish(far, one, two, basis, near):
    out = shaped((R, LEAF_DEV * LEAF), F32)
    return call(finish_kernel, 4, out, (), (far, one, two, basis, near))


def tables(neighbours, far_lists, x, z, c, group):
    offsets = jnp.asarray(OFFSETS, jnp.int32)
    there = (z + offsets + NZ) % NZ
    row_near = lax.dynamic_index_in_dim(
        neighbours.reshape(NX, NZ, NC, LEAF_DEV * NB), z, 1, keepdims=False
    ).reshape(GROUP, LEAF_DEV * NB)
    row_far = lax.dynamic_index_in_dim(
        far_lists.reshape(NX, NZ, NC, NODE_DEV * FAR), z, 1, keepdims=False
    ).reshape(GROUP, NODE_DEV * FAR)
    remote = jnp.arange(LEAF_DEV * NB, dtype=jnp.int32) % NB > 0
    near_owner = jnp.where(remote, row_near // LEAF_DEV, -1)
    far_owner = row_far // NODE_DEV
    mine = (x * NZ + there) * NC + c

    def pick(owner, value, sources):
        hit = owner[:, None, :] == sources[:, :, None]
        return jnp.sum(jnp.where(hit, value[:, None, :], 0), axis=2, dtype=jnp.int32)

    send_sources = jnp.broadcast_to(mine[None, :], (GROUP, NZ))
    send_leaf = pick(near_owner, row_near % LEAF_DEV, send_sources)
    send_node = pick(far_owner, row_far % NODE_DEV, send_sources)
    member = jnp.arange(GROUP, dtype=jnp.int32)
    seen = ((member // NC)[:, None] * NZ + there[None, :]) * NC + (member % NC)[:, None]
    own_near = lax.dynamic_index_in_dim(near_owner, group, 0, keepdims=True)
    own_far = lax.dynamic_index_in_dim(far_owner, group, 0, keepdims=True)
    near_value = jnp.arange(LEAF_DEV * NB, dtype=jnp.int32)[None, :] // NB + 1
    far_value = jnp.arange(NODE_DEV * FAR, dtype=jnp.int32)[None, :] + 1
    take_leaf = pick(own_near, near_value, seen) - 1
    take_node = pick(own_far, far_value, seen) - 1
    return send_leaf, send_node, take_leaf, take_node


def shift(value, step):
    return lax.ppermute(value, "leaf", ring(step))


def travel(payload, half):
    arrived = [(payload,)]
    up, down = payload, payload
    for _ in range(1, NZ // 2):
        up = shift(up, 1)
        down = shift(down, -1)
        arrived += [(up,), (down,)]
    last_up = shift(up[:half], 1)
    last_down = shift(down[half:], -1)
    arrived.append((last_up, last_down))
    return arrived


def exchange(chosen):
    return lax.all_to_all(
        chosen, "leaf", split_axis=0, concat_axis=0, axis_index_groups=ROW_GROUPS, tiled=True
    )


def join_planes(quarter):
    joined = []
    for step in (1, NY - 1, 2):
        joined.append(lax.ppermute(quarter, "rhs", [(i, (i + step) % NY) for i in range(NY)]))
    return joined


def on_device(coords, rhs, basis, transfer_one, transfer_two, far_blocks, neighbours, far_lists):
    me = lax.axis_index("leaf").astype(jnp.int32)
    y = lax.axis_index("rhs").astype(jnp.int32).reshape(1)
    c, z, x = me % NC, (me // NC) % NZ, me // (NC * NZ)
    group = x * NC + c
    payload = pack(y, rhs, coords)
    leaves = travel(payload, LEAF_DEV // 2)
    nodes = travel(skeletons(payload, basis, transfer_one, transfer_two), NODE_DEV // 2)
    send_leaf, send_node, take_leaf, take_node = tables(neighbours, far_lists, x, z, c, group)
    targets, near = own_tiles(y, rhs, coords)
    blocks = far_blocks.reshape(NODE_DEV * FAR, RANK, RANK)
    far = None
    for chunks in LEAF_CHUNKS:
        got = [exchange(choose(low, send_leaf, leaves[low:high])) for low, high in chunks]
        quarter = [part[:, :, R:, :] for part in got]
        quarter = quarter[0] if len(quarter) == 1 else jnp.concatenate(quarter, axis=1)
        others = join_planes(quarter)
        near = near_chunk(chunks, take_leaf, got, others, targets, near)
    for low, high in NODE_CHUNKS:
        got = exchange(choose(low, send_node, nodes[low:high]))
        far = far_chunk(low, high, take_node, got, blocks, far)
    return finish(far, transfer_one, transfer_two, basis, near)


def solution(mesh):
    return jax.shard_map(
        on_device,
        mesh=mesh,
        in_specs=(
            P(None, "leaf"),
            P("rhs", "leaf"),
            P("leaf", None, None),
            P("leaf", None, None),
            P("leaf", None, None),
            P("leaf", None, None, None),
            P(),
            P(),
        ),
        out_specs=P("rhs", "leaf"),
        check_vma=False,
    )
```

```python
import functools

import jax
import jax.numpy as jnp
from jax import lax
from jax.experimental import pallas as pl
from jax.experimental.pallas import tpu as pltpu
from jax.sharding import PartitionSpec as P


FEAT = 64
RANK = 256
R = 64
LEAF = 512
NB = 8
FAR = 4
NX, NZ, NC, NY = 4, 8, 2, 4
GROUP = NX * NC
LEAF_DEV = 8
NODE_DEV = 14
QUART = FEAT // NY
ROWS = R + QUART
AUG = 128
OFFSETS = (0, -1, 1, -2, 2, -3, 3, 4)
LEAF_CHUNKS = (((0, 3), (3, 5)), ((5, 7), (7, 8)))


F32 = jnp.float32
BF16 = jnp.bfloat16


def place(x, z, c):
    return (x * NZ + z % NZ) * NC + c


def ring(step):
    return [
        (place(x, z, c), place(x, z + step, c))
        for x in range(NX)
        for z in range(NZ)
        for c in range(NC)
    ]


def across(step):
    return [
        (place(x, z, c), place((x + step) % NX, z, c))
        for x in range(NX)
        for z in range(NZ)
        for c in range(NC)
    ]


FLIP = [(place(x, z, c), place(x, z, 1 - c)) for x in range(NX) for z in range(NZ) for c in range(NC)]
ROW_GROUPS = [[place(x, z, c) for x in range(NX) for c in range(NC)] for z in range(NZ)]


def cost(micros):
    return pl.CostEstimate(flops=int(micros * 1e9), bytes_accessed=0, transcendentals=0)


VMEM = pl.BlockSpec(memory_space=pltpu.VMEM)
SMEM = pl.BlockSpec(memory_space=pltpu.SMEM)


def call(kernel, micros, out, tables, arrays, scratch=(), megabytes=16):
    return pl.pallas_call(
        kernel,
        in_specs=[SMEM] * len(tables) + [VMEM] * len(arrays),
        out_specs=jax.tree.map(lambda _: VMEM, out),
        out_shape=out,
        scratch_shapes=list(scratch),
        compiler_params=pltpu.CompilerParams(vmem_limit_bytes=megabytes << 20),
        cost_estimate=cost(micros),
    )(*tables, *arrays)


def shaped(shape, kind):
    return jax.ShapeDtypeStruct(shape, kind)


def nt(a, b):
    return lax.dot_general(a, b, (((1,), (1,)), ((), ())), preferred_element_type=F32)


def pack_kernel(y_ref, rhs_ref, coords_ref, out_ref):
    start = pl.multiple_of(y_ref[0] * QUART, QUART)
    for leaf in range(LEAF_DEV):
        columns = slice(leaf * LEAF, (leaf + 1) * LEAF)
        out_ref[leaf, :R, :] = rhs_ref[:, columns]
        out_ref[leaf, R:, :] = coords_ref[pl.ds(start, QUART), columns]


def pack(y, rhs, coords):
    out = shaped((LEAF_DEV, ROWS, LEAF), BF16)
    return call(pack_kernel, 1, out, (y,), (rhs, coords), megabytes=8)


def square_rows(pieces, source):
    total = None
    for piece in pieces:
        wide = piece.astype(F32)
        part = jnp.sum(wide * wide, axis=0, keepdims=True)
        total = part if total is None else total + part
    total = total * -0.5
    high = total.astype(BF16).astype(F32)
    rest = total - high
    middle = rest.astype(BF16).astype(F32)
    low = rest - middle
    row = lax.broadcasted_iota(jnp.int32, (16, LEAF), 0)
    own = row if source else row - 3
    other = row - 3 if source else row
    block = jnp.where(own == 0, high, jnp.where(own == 1, middle, jnp.where(own == 2, low, 0.0)))
    block = jnp.where(jnp.logical_and(other >= 0, other < 3), 1.0, block)
    return block.astype(BF16)


def tile_product(target, spread, charges):
    exponent = jnp.dot(target, spread, preferred_element_type=F32)
    return nt(jnp.exp(exponent).astype(BF16), charges)


def own_kernel(pos_ref, rhs_ref, coords_ref, other_ref, target_ref, near_ref, spread_ref):
    y = pos_ref[0]
    empty = jnp.zeros((AUG - FEAT - 16, LEAF), BF16)
    for core, ref in enumerate((coords_ref, other_ref)):
        for leaf in range(LEAF_DEV):
            columns = slice(leaf * LEAF, (leaf + 1) * LEAF)
            pieces = []
            for shift_by in (0, NY - 1, 1, 2):
                start = pl.multiple_of(lax.rem(y + shift_by, NY) * QUART, QUART)
                pieces.append(ref[pl.ds(start, QUART), columns])
            wide = jnp.concatenate(pieces + [square_rows(pieces, False), empty], axis=0)
            target_ref[core * LEAF_DEV + leaf] = wide.astype(F32).T.astype(BF16)
            if core == 0:
                spread_ref[leaf, :FEAT, :] = jnp.concatenate(pieces, axis=0)
                spread_ref[leaf, FEAT : FEAT + 16, :] = square_rows(pieces, True)
                spread_ref[leaf, FEAT + 16 :, :] = empty

    def pair(i, carry):
        for leaf in (2 * i, 2 * i + 1):
            charges = rhs_ref[:, pl.ds(pl.multiple_of(leaf * LEAF, LEAF), LEAF)]
            product = tile_product(target_ref[leaf], spread_ref[leaf], charges)
            near_ref[:, pl.ds(pl.multiple_of(leaf * LEAF, LEAF), LEAF)] = product.T
        return carry

    lax.fori_loop(0, LEAF_DEV // 2, pair, 0)


def own_tiles(pos, rhs, coords, other):
    out = [shaped((2 * LEAF_DEV, LEAF, AUG), BF16), shaped((R, LEAF_DEV * LEAF), F32)]
    scratch = [pltpu.VMEM((LEAF_DEV, AUG, LEAF), BF16)]
    return call(own_kernel, 5, out, (pos,), (rhs, coords, other), scratch, 20)


UNROLL = 4


def near_kernel(chunks, take_ref, *refs):
    given = NX * len(chunks)
    got_refs, piece_refs = refs[:given], refs[given : given + NY]
    target_ref, *before_refs = refs[given + NY : -5]
    own_ref, other_ref, spread_ref, held_ref, near_ref = refs[-5:]
    near_ref[...] = jnp.zeros_like(near_ref)
    spread_ref[:, FEAT + 16 :, :] = jnp.zeros((UNROLL, AUG - FEAT - 16, LEAF), BF16)
    start, slots = chunks[0][0], chunks[-1][1] - chunks[0][0]
    for index, (low, high) in enumerate(chunks):
        for step in range(NX):
            for side in range(NC):
                block = got_refs[NX * index + step][side, :, :R, :]
                held_ref[NC * step + side, low - start : high - start] = block

    def some(i, carry):
        for buffer in range(UNROLL):
            item = i * UNROLL + buffer
            source, slot = item // slots, item % slots
            which = take_ref[source, start + slot]
            pieces = [ref[source, slot] for ref in piece_refs]
            for q, piece in enumerate(pieces):
                spread_ref[buffer, q * QUART : (q + 1) * QUART, :] = piece
            spread_ref[buffer, FEAT : FEAT + 16, :] = square_rows(pieces, True)
            charges = held_ref[source, slot]
            charges = jnp.where(which >= 0, charges, jnp.zeros_like(charges))
            leaf = jnp.maximum(which, 0)
            near_ref[leaf] += tile_product(target_ref[leaf], spread_ref[buffer], charges)
        return carry

    lax.fori_loop(0, GROUP * slots // UNROLL, some, 0)
    for core, out_ref in enumerate((own_ref, other_ref)):
        for leaf in range(LEAF_DEV):
            columns = slice(leaf * LEAF, (leaf + 1) * LEAF)
            near = near_ref[core * LEAF_DEV + leaf].T
            out_ref[:, columns] = near + before_refs[core][:, columns] if before_refs else near


def near_chunk(chunks, take, got, pieces, targets, before):
    slots = chunks[-1][1] - chunks[0][0]
    flat = shaped((R, LEAF_DEV * LEAF), F32)
    return call(
        functools.partial(near_kernel, chunks),
        3.2 * slots,
        [flat, flat],
        (take,),
        (*got, *pieces, targets, *before),
        [
            pltpu.VMEM((UNROLL, AUG, LEAF), BF16),
            pltpu.VMEM((GROUP, slots, R, LEAF), BF16),
            pltpu.VMEM((2 * LEAF_DEV, LEAF, R), F32),
        ],
        40,
    )


def quarter_kernel(*refs):
    out_ref = refs[-1]
    at = 0
    for first in range(0, len(refs) - 1, NX):
        count = refs[first].shape[1]
        for step in range(NX):
            for side in range(NC):
                out_ref[NC * step + side, at : at + count] = refs[first + step][side, :, R:, :]
        at += count


def quarters(got):
    slots = sum(part.shape[1] for part in got[::NX])
    out = shaped((GROUP, slots, QUART, LEAF), BF16)
    return call(quarter_kernel, 1, out, (), got, megabytes=16)


def choose_kernel(first, send_ref, *refs):
    out_ref = refs[-1]
    for slot, ref in enumerate(refs[:-1]):
        for target in range(GROUP):
            out_ref[target, slot] = ref[send_ref[target, first + slot]]


def choose_steps_kernel(first, send_ref, *refs):
    sources, outs = refs[:-NX], refs[-NX:]
    for slot, ref in enumerate(sources):
        for step in range(NX):
            for side in range(NC):
                outs[step][side, slot] = ref[send_ref[NC * step + side, first + slot]]


def choose(first, send, sources, kind):
    shape = sources[0].shape[1:]
    count = len(sources)
    if kind == "leaf":
        kernel, out = choose_steps_kernel, [shaped((NC, count, *shape), BF16)] * NX
    else:
        kernel, out = choose_kernel, shaped((GROUP, count, *shape), BF16)
    kernel = functools.partial(kernel, first)
    return call(kernel, 1, out, (send,), sources)


def skeleton_kernel(leaves_ref, basis_ref, one_ref, two_ref, out_ref):
    def rounded_dot(a, b):
        return jnp.dot(a, b, preferred_element_type=F32).astype(BF16)

    for leaf in range(LEAF_DEV):
        out_ref[leaf] = rounded_dot(leaves_ref[leaf, :R, :], basis_ref[leaf])
    for m in range(LEAF_DEV // 2):
        joined = jnp.concatenate([out_ref[2 * m], out_ref[2 * m + 1]], axis=1)
        out_ref[LEAF_DEV + m] = rounded_dot(joined, one_ref[m])
    for m in range(LEAF_DEV // 4):
        low = LEAF_DEV + 2 * m
        joined = jnp.concatenate([out_ref[low], out_ref[low + 1]], axis=1)
        out_ref[LEAF_DEV * 3 // 2 + m] = rounded_dot(joined, two_ref[m])


def skeletons(leaves, basis, one, two):
    out = shaped((NODE_DEV, R, RANK), BF16)
    return call(skeleton_kernel, 3, out, (), (leaves, basis, one, two))


def far_kernel(take_ref, got_ref, blocks_ref, out_ref, held_ref, sems):
    out_ref[...] = jnp.zeros_like(out_ref)

    def fetch(i):
        at = jnp.maximum(take_ref[i // NZ, i % NZ], 0)
        return pltpu.make_async_copy(blocks_ref.at[at], held_ref.at[i], sems.at[i])

    def begin(i, carry):
        fetch(i).start()
        return carry

    lax.fori_loop(0, GROUP * NZ, begin, 0)

    def source_of(source, carry):
        for slot in range(NZ):
            item = source * NZ + slot
            which = take_ref[source, slot]
            weights = got_ref[source, slot]
            weights = jnp.where(which >= 0, weights, jnp.zeros_like(weights))
            fetch(item).wait()
            out_ref[jnp.maximum(which, 0) // FAR] += jnp.dot(
                weights, held_ref[item], preferred_element_type=F32
            )
        return carry

    lax.fori_loop(0, GROUP, source_of, 0)


def far_part(take, got, blocks):
    return pl.pallas_call(
        far_kernel,
        in_specs=[SMEM, VMEM, pl.BlockSpec(memory_space=pltpu.HBM)],
        out_specs=VMEM,
        out_shape=shaped((NODE_DEV, R, RANK), F32),
        scratch_shapes=[
            pltpu.VMEM((GROUP * NZ, RANK, RANK), BF16),
            pltpu.SemaphoreType.DMA((GROUP * NZ,)),
        ],
        compiler_params=pltpu.CompilerParams(vmem_limit_bytes=20 << 20),
        cost_estimate=cost(5),
        name="far_part",
    )(take, got, blocks)


def finish_kernel(far_ref, one_ref, two_ref, basis_ref, self_ref, own_ref, other_ref, out_ref):
    for m in range(LEAF_DEV // 4):
        spread = nt(far_ref[LEAF_DEV * 3 // 2 + m].astype(BF16), two_ref[m])
        for side in range(2):
            node = 2 * m + side
            middle = far_ref[LEAF_DEV + node] + spread[:, side * RANK : (side + 1) * RANK]
            lower = nt(middle.astype(BF16), one_ref[node])
            for part in range(2):
                leaf = 2 * node + part
                lowest = far_ref[leaf] + lower[:, part * RANK : (part + 1) * RANK]
                columns = slice(leaf * LEAF, (leaf + 1) * LEAF)
                near = self_ref[:, columns] + own_ref[:, columns] + other_ref[:, columns]
                out_ref[:, columns] = near + nt(lowest.astype(BF16), basis_ref[leaf])


def finish(far, one, two, basis, *near):
    out = shaped((R, LEAF_DEV * LEAF), F32)
    return call(finish_kernel, 4, out, (), (far, one, two, basis, *near), megabytes=20)


def tables(neighbours, far_lists, x, z, c, group):
    offsets = jnp.asarray(OFFSETS, jnp.int32)
    there = (z + offsets + NZ) % NZ
    row_near = lax.dynamic_index_in_dim(
        neighbours.reshape(NX, NZ, NC, LEAF_DEV * NB), z, 1, keepdims=False
    ).reshape(GROUP, LEAF_DEV * NB)
    row_far = lax.dynamic_index_in_dim(
        far_lists.reshape(NX, NZ, NC, NODE_DEV * FAR), z, 1, keepdims=False
    ).reshape(GROUP, NODE_DEV * FAR)
    remote = jnp.arange(LEAF_DEV * NB, dtype=jnp.int32) % NB > 0
    near_owner = jnp.where(remote, row_near // LEAF_DEV, -1)
    far_owner = row_far // NODE_DEV
    mine = (x * NZ + there) * NC + c

    def pick(owner, value, sources):
        hit = owner[:, None, :] == sources[:, :, None]
        return jnp.sum(jnp.where(hit, value[:, None, :], 0), axis=2, dtype=jnp.int32)

    member = jnp.arange(GROUP, dtype=jnp.int32)
    sent_from = jnp.broadcast_to(mine[None, :], (GROUP, NZ))
    step, side = member // NC, member % NC
    core = jnp.where(side == 0, c, 1 - c)
    to_row = (x + step) % NX * NC + core
    send_leaf = pick(near_owner[to_row], row_near[to_row] % LEAF_DEV, sent_from)
    send_node = pick(far_owner, row_far % NODE_DEV, sent_from)
    came_from = (((x - step + NX) % NX)[:, None] * NZ + there[None, :]) * NC + c
    near_value = jnp.arange(LEAF_DEV * NB, dtype=jnp.int32)[None, :] // NB + 1
    near_value = near_value + side[:, None] * LEAF_DEV
    take_leaf = pick(near_owner[x * NC + core], near_value, came_from) - 1
    seen = ((member // NC)[:, None] * NZ + there[None, :]) * NC + (member % NC)[:, None]
    own_far = lax.dynamic_index_in_dim(far_owner, group, 0, keepdims=True)
    far_value = jnp.arange(NODE_DEV * FAR, dtype=jnp.int32)[None, :] + 1
    take_node = pick(own_far, far_value, seen) - 1
    return send_leaf, send_node, take_leaf, take_node


def shift(value, step):
    return lax.ppermute(value, "leaf", ring(step))


def travel(payload, last):
    arrived = [payload]
    up, down = payload, payload
    for _ in range(1, NZ // 2):
        up = shift(up, 1)
        down = shift(down, -1)
        arrived += [up, down]
    arrived.append(shift(up if last == 1 else down, last))
    return arrived


def cross(chosen):
    got = [chosen[0]]
    for step in range(1, NX):
        got.append(lax.ppermute(chosen[step], "leaf", across(step)))
    return got


def flip(value):
    return lax.ppermute(value, "leaf", FLIP)


def exchange(chosen):
    return lax.all_to_all(
        chosen, "leaf", split_axis=0, concat_axis=0, axis_index_groups=ROW_GROUPS, tiled=True
    )


def join_planes(quarter):
    joined = []
    for step in (1, NY - 1, 2):
        joined.append(lax.ppermute(quarter, "rhs", [(i, (i + step) % NY) for i in range(NY)]))
    return joined


def on_device(coords, rhs, basis, transfer_one, transfer_two, far_blocks, neighbours, far_lists):
    me = lax.axis_index("leaf").astype(jnp.int32)
    y = lax.axis_index("rhs").astype(jnp.int32).reshape(1)
    c, z, x = me % NC, (me // NC) % NZ, me // (NC * NZ)
    group = x * NC + c
    payload = pack(y, rhs, coords)
    other_coords = flip(coords)
    leaves = travel(payload, 1)
    nodes = travel(skeletons(payload, basis, transfer_one, transfer_two), -1)
    send_leaf, send_node, take_leaf, take_node = tables(neighbours, far_lists, x, z, c, group)
    targets, self_part = own_tiles(y, rhs, coords, other_coords)
    near = ()
    for chunks in LEAF_CHUNKS:
        got = []
        for low, high in chunks:
            got += cross(choose(low, send_leaf, leaves[low:high], "leaf"))
        quarter = quarters(got)
        pieces = [quarter] + join_planes(quarter)
        near = near_chunk(chunks, take_leaf, got, pieces, targets, near)
    own, other = near
    other = flip(other)
    got = exchange(choose(0, send_node, nodes, "node"))
    far = far_part(take_node, got, far_blocks.reshape(NODE_DEV * FAR, RANK, RANK))
    return finish(far, transfer_one, transfer_two, basis, self_part, own, other)


def solution(mesh):
    return jax.shard_map(
        on_device,
        mesh=mesh,
        in_specs=(
            P(None, "leaf"),
            P("rhs", "leaf"),
            P("leaf", None, None),
            P("leaf", None, None),
            P("leaf", None, None),
            P("leaf", None, None, None),
            P(),
            P(),
        ),
        out_specs=P("rhs", "leaf"),
        check_vma=False,
    )
```

```python
import functools

import jax
import jax.numpy as jnp
from jax import lax
from jax.experimental import pallas as pl
from jax.experimental.pallas import tpu as pltpu
from jax.sharding import PartitionSpec as P


FEAT = 64
RANK = 256
R = 64
LEAF = 512
NB = 8
FAR = 4
NX, NZ, NC, NY = 4, 8, 2, 4
GROUP = NX * NC
LEAF_DEV = 8
NODE_DEV = 14
QUART = FEAT // NY
ROWS = R + QUART
AUG = 128
OFFSETS = (0, -1, 1, -2, 2, -3, 3, 4)
LEAF_CHUNKS = (((0, 3),), ((3, 5), (5, 7)), ((7, 8),))


F32 = jnp.float32
BF16 = jnp.bfloat16


def place(x, z, c):
    return (x * NZ + z % NZ) * NC + c


def ring(step):
    return [
        (place(x, z, c), place(x, z + step, c))
        for x in range(NX)
        for z in range(NZ)
        for c in range(NC)
    ]


def across(step):
    return [
        (place(x, z, c), place((x + step) % NX, z, c))
        for x in range(NX)
        for z in range(NZ)
        for c in range(NC)
    ]


FLIP = [(place(x, z, c), place(x, z, 1 - c)) for x in range(NX) for z in range(NZ) for c in range(NC)]
ROW_GROUPS = [[place(x, z, c) for x in range(NX) for c in range(NC)] for z in range(NZ)]


def cost(micros):
    return pl.CostEstimate(flops=int(micros * 1e9), bytes_accessed=0, transcendentals=0)


VMEM = pl.BlockSpec(memory_space=pltpu.VMEM)
SMEM = pl.BlockSpec(memory_space=pltpu.SMEM)


def call(kernel, micros, out, tables, arrays, scratch=(), megabytes=16):
    return pl.pallas_call(
        kernel,
        in_specs=[SMEM] * len(tables) + [VMEM] * len(arrays),
        out_specs=jax.tree.map(lambda _: VMEM, out),
        out_shape=out,
        scratch_shapes=list(scratch),
        compiler_params=pltpu.CompilerParams(vmem_limit_bytes=megabytes << 20),
        cost_estimate=cost(micros),
    )(*tables, *arrays)


def shaped(shape, kind):
    return jax.ShapeDtypeStruct(shape, kind)


def nt(a, b):
    return lax.dot_general(a, b, (((1,), (1,)), ((), ())), preferred_element_type=F32)


def pack_kernel(y_ref, rhs_ref, coords_ref, out_ref):
    start = pl.multiple_of(y_ref[0] * QUART, QUART)
    for leaf in range(LEAF_DEV):
        columns = slice(leaf * LEAF, (leaf + 1) * LEAF)
        out_ref[leaf, :R, :] = rhs_ref[:, columns]
        out_ref[leaf, R:, :] = coords_ref[pl.ds(start, QUART), columns]


def pack(y, rhs, coords):
    out = shaped((LEAF_DEV, ROWS, LEAF), BF16)
    return call(pack_kernel, 1, out, (y,), (rhs, coords), megabytes=8)


def square_rows(pieces, source):
    total = None
    for piece in pieces:
        wide = piece.astype(F32)
        part = jnp.sum(wide * wide, axis=0, keepdims=True)
        total = part if total is None else total + part
    total = total * -0.5
    high = total.astype(BF16).astype(F32)
    rest = total - high
    middle = rest.astype(BF16).astype(F32)
    low = rest - middle
    row = lax.broadcasted_iota(jnp.int32, (16, LEAF), 0)
    own = row if source else row - 3
    other = row - 3 if source else row
    block = jnp.where(own == 0, high, jnp.where(own == 1, middle, jnp.where(own == 2, low, 0.0)))
    block = jnp.where(jnp.logical_and(other >= 0, other < 3), 1.0, block)
    return block.astype(BF16)


def tile_product(target, spread, charges):
    exponent = jnp.dot(target, spread, preferred_element_type=F32)
    return nt(jnp.exp(exponent).astype(BF16), charges)


def own_kernel(pos_ref, rhs_ref, coords_ref, other_ref, target_ref, near_ref, spread_ref):
    y = pos_ref[0]
    empty = jnp.zeros((AUG - FEAT - 16, LEAF), BF16)

    def spread_leaf(leaf, carry):
        columns = pl.ds(pl.multiple_of(leaf * LEAF, LEAF), LEAF)
        for core, ref in enumerate((coords_ref, other_ref)):
            pieces = []
            for shift_by in (0, NY - 1, 1, 2):
                start = pl.multiple_of(lax.rem(y + shift_by, NY) * QUART, QUART)
                pieces.append(ref[pl.ds(start, QUART), columns])
            wide = jnp.concatenate(pieces + [square_rows(pieces, False), empty], axis=0)
            target_ref[core * LEAF_DEV + leaf] = wide.astype(F32).T.astype(BF16)
            if core == 0:
                spread_ref[leaf, :FEAT, :] = jnp.concatenate(pieces, axis=0)
                spread_ref[leaf, FEAT : FEAT + 16, :] = square_rows(pieces, True)
                spread_ref[leaf, FEAT + 16 :, :] = empty
        return carry

    lax.fori_loop(0, LEAF_DEV, spread_leaf, 0)

    def pair(i, carry):
        for leaf in (2 * i, 2 * i + 1):
            charges = rhs_ref[:, pl.ds(pl.multiple_of(leaf * LEAF, LEAF), LEAF)]
            product = tile_product(target_ref[leaf], spread_ref[leaf], charges)
            near_ref[:, pl.ds(pl.multiple_of(leaf * LEAF, LEAF), LEAF)] = product.T
        return carry

    lax.fori_loop(0, LEAF_DEV // 2, pair, 0)


def own_tiles(pos, rhs, coords, other):
    out = [shaped((2 * LEAF_DEV, LEAF, AUG), BF16), shaped((R, LEAF_DEV * LEAF), F32)]
    scratch = [pltpu.VMEM((LEAF_DEV, AUG, LEAF), BF16)]
    return call(own_kernel, 5, out, (pos,), (rhs, coords, other), scratch, 20)


UNROLL = 4


def near_kernel(chunks, take_ref, *refs):
    given = NX * len(chunks)
    got_refs, piece_refs = refs[:given], refs[given : given + NY]
    target_ref, *before_refs = refs[given + NY : -5]
    own_ref, other_ref, spread_ref, held_ref, near_ref = refs[-5:]
    near_ref[...] = jnp.zeros_like(near_ref)
    spread_ref[:, FEAT + 16 :, :] = jnp.zeros((UNROLL, AUG - FEAT - 16, LEAF), BF16)
    start, slots = chunks[0][0], chunks[-1][1] - chunks[0][0]
    for index, (low, high) in enumerate(chunks):
        for step in range(NX):
            for side in range(NC):
                block = got_refs[NX * index + step][side, :, :R, :]
                held_ref[NC * step + side, low - start : high - start] = block

    def some(i, carry):
        for buffer in range(UNROLL):
            item = i * UNROLL + buffer
            source, slot = item // slots, item % slots
            which = take_ref[source, start + slot]
            pieces = [ref[source, slot] for ref in piece_refs]
            for q, piece in enumerate(pieces):
                spread_ref[buffer, q * QUART : (q + 1) * QUART, :] = piece
            spread_ref[buffer, FEAT : FEAT + 16, :] = square_rows(pieces, True)
            charges = held_ref[source, slot]
            charges = jnp.where(which >= 0, charges, jnp.zeros_like(charges))
            leaf = jnp.maximum(which, 0)
            near_ref[leaf] += tile_product(target_ref[leaf], spread_ref[buffer], charges)
        return carry

    lax.fori_loop(0, GROUP * slots // UNROLL, some, 0)

    def emit(leaf, carry):
        columns = pl.ds(pl.multiple_of(leaf * LEAF, LEAF), LEAF)
        for core, out_ref in enumerate((own_ref, other_ref)):
            near = near_ref[core * LEAF_DEV + leaf].T
            out_ref[:, columns] = near + before_refs[core][:, columns] if before_refs else near
        return carry

    lax.fori_loop(0, LEAF_DEV, emit, 0)


def near_chunk(chunks, take, got, pieces, targets, before):
    slots = chunks[-1][1] - chunks[0][0]
    flat = shaped((R, LEAF_DEV * LEAF), F32)
    return call(
        functools.partial(near_kernel, chunks),
        3.2 * slots,
        [flat, flat],
        (take,),
        (*got, *pieces, targets, *before),
        [
            pltpu.VMEM((UNROLL, AUG, LEAF), BF16),
            pltpu.VMEM((GROUP, slots, R, LEAF), BF16),
            pltpu.VMEM((2 * LEAF_DEV, LEAF, R), F32),
        ],
        28,
    )


def quarter_kernel(*refs):
    out_ref = refs[-1]
    at = 0
    for first in range(0, len(refs) - 1, NX):
        count = refs[first].shape[1]
        for step in range(NX):
            for side in range(NC):
                out_ref[NC * step + side, at : at + count] = refs[first + step][side, :, R:, :]
        at += count


def quarters(got):
    slots = sum(part.shape[1] for part in got[::NX])
    out = shaped((GROUP, slots, QUART, LEAF), BF16)
    return call(quarter_kernel, 1, out, (), got, megabytes=16)


def choose_kernel(first, send_ref, *refs):
    out_ref = refs[-1]

    def fill(target, carry):
        for slot, ref in enumerate(refs[:-1]):
            out_ref[target, slot] = ref[send_ref[target, first + slot]]
        return carry

    lax.fori_loop(0, GROUP, fill, 0)


def choose_steps_kernel(first, send_ref, *refs):
    sources, outs = refs[:-NX], refs[-NX:]

    def fill(side, carry):
        for slot, ref in enumerate(sources):
            for step in range(NX):
                outs[step][side, slot] = ref[send_ref[NC * step + side, first + slot]]
        return carry

    lax.fori_loop(0, NC, fill, 0)


def choose(first, send, sources, kind):
    shape = sources[0].shape[1:]
    count = len(sources)
    if kind == "leaf":
        kernel, out = choose_steps_kernel, [shaped((NC, count, *shape), BF16)] * NX
    else:
        kernel, out = choose_kernel, shaped((GROUP, count, *shape), BF16)
    kernel = functools.partial(kernel, first)
    return call(kernel, 1, out, (send,), sources)


def skeleton_kernel(leaves_ref, basis_ref, one_ref, two_ref, out_ref):
    def rounded_dot(a, b):
        return jnp.dot(a, b, preferred_element_type=F32).astype(BF16)

    for leaf in range(LEAF_DEV):
        out_ref[leaf] = rounded_dot(leaves_ref[leaf, :R, :], basis_ref[leaf])
    for m in range(LEAF_DEV // 2):
        joined = jnp.concatenate([out_ref[2 * m], out_ref[2 * m + 1]], axis=1)
        out_ref[LEAF_DEV + m] = rounded_dot(joined, one_ref[m])
    for m in range(LEAF_DEV // 4):
        low = LEAF_DEV + 2 * m
        joined = jnp.concatenate([out_ref[low], out_ref[low + 1]], axis=1)
        out_ref[LEAF_DEV * 3 // 2 + m] = rounded_dot(joined, two_ref[m])


def skeletons(leaves, basis, one, two):
    out = shaped((NODE_DEV, R, RANK), BF16)
    return call(skeleton_kernel, 3, out, (), (leaves, basis, one, two))


def far_kernel(take_ref, got_ref, blocks_ref, out_ref):
    out_ref[...] = jnp.zeros_like(out_ref)

    def some(i, carry):
        for buffer in range(UNROLL):
            item = i * UNROLL + buffer
            source, slot = item // NZ, item % NZ
            which = take_ref[source, slot]
            weights = got_ref[source, slot]
            weights = jnp.where(which >= 0, weights, jnp.zeros_like(weights))
            at = jnp.maximum(which, 0)
            out_ref[at // FAR] += jnp.dot(weights, blocks_ref[at], preferred_element_type=F32)
        return carry

    lax.fori_loop(0, GROUP * NZ // UNROLL, some, 0)


def far_part(take, got, blocks):
    out = shaped((NODE_DEV, R, RANK), F32)
    return call(far_kernel, 5, out, (take,), (got, blocks))


def finish_kernel(far_ref, one_ref, two_ref, basis_ref, self_ref, own_ref, other_ref, out_ref, low_ref):
    for m in range(LEAF_DEV // 4):
        spread = nt(far_ref[LEAF_DEV * 3 // 2 + m].astype(BF16), two_ref[m])
        for side in range(2):
            node = 2 * m + side
            middle = far_ref[LEAF_DEV + node] + spread[:, side * RANK : (side + 1) * RANK]
            lower = nt(middle.astype(BF16), one_ref[node])
            for part in range(2):
                leaf = 2 * node + part
                lowest = far_ref[leaf] + lower[:, part * RANK : (part + 1) * RANK]
                low_ref[leaf] = lowest.astype(BF16)

    def emit(i, carry):
        for leaf in (2 * i, 2 * i + 1):
            columns = pl.ds(pl.multiple_of(leaf * LEAF, LEAF), LEAF)
            near = self_ref[:, columns] + own_ref[:, columns] + other_ref[:, columns]
            out_ref[:, columns] = near + nt(low_ref[leaf], basis_ref[leaf])
        return carry

    lax.fori_loop(0, LEAF_DEV // 2, emit, 0)


def finish(far, one, two, basis, *near):
    out = shaped((R, LEAF_DEV * LEAF), F32)
    scratch = [pltpu.VMEM((LEAF_DEV, R, RANK), BF16)]
    return call(finish_kernel, 4, out, (), (far, one, two, basis, *near), scratch, 20)


def tables(neighbours, far_lists, x, z, c, group):
    offsets = jnp.asarray(OFFSETS, jnp.int32)
    there = (z + offsets + NZ) % NZ
    row_near = lax.dynamic_index_in_dim(
        neighbours.reshape(NX, NZ, NC, LEAF_DEV * NB), z, 1, keepdims=False
    ).reshape(GROUP, LEAF_DEV * NB)
    row_far = lax.dynamic_index_in_dim(
        far_lists.reshape(NX, NZ, NC, NODE_DEV * FAR), z, 1, keepdims=False
    ).reshape(GROUP, NODE_DEV * FAR)
    remote = jnp.arange(LEAF_DEV * NB, dtype=jnp.int32) % NB > 0
    near_owner = jnp.where(remote, row_near // LEAF_DEV, -1)
    far_owner = row_far // NODE_DEV
    mine = (x * NZ + there) * NC + c

    def pick(owner, value, sources):
        hit = owner[:, None, :] == sources[:, :, None]
        return jnp.sum(jnp.where(hit, value[:, None, :], 0), axis=2, dtype=jnp.int32)

    member = jnp.arange(GROUP, dtype=jnp.int32)
    sent_from = jnp.broadcast_to(mine[None, :], (GROUP, NZ))
    step, side = member // NC, member % NC
    core = jnp.where(side == 0, c, 1 - c)
    to_row = (x + step) % NX * NC + core
    send_leaf = pick(near_owner[to_row], row_near[to_row] % LEAF_DEV, sent_from)
    send_node = pick(far_owner, row_far % NODE_DEV, sent_from)
    came_from = (((x - step + NX) % NX)[:, None] * NZ + there[None, :]) * NC + c
    near_value = jnp.arange(LEAF_DEV * NB, dtype=jnp.int32)[None, :] // NB + 1
    near_value = near_value + side[:, None] * LEAF_DEV
    take_leaf = pick(near_owner[x * NC + core], near_value, came_from) - 1
    seen = ((member // NC)[:, None] * NZ + there[None, :]) * NC + (member % NC)[:, None]
    own_far = lax.dynamic_index_in_dim(far_owner, group, 0, keepdims=True)
    far_value = jnp.arange(NODE_DEV * FAR, dtype=jnp.int32)[None, :] + 1
    take_node = pick(own_far, far_value, seen) - 1
    return send_leaf, send_node, take_leaf, take_node


def shift(value, step):
    return lax.ppermute(value, "leaf", ring(step))


def travel(payload, last):
    arrived = [payload]
    up, down = payload, payload
    for _ in range(1, NZ // 2):
        up = shift(up, 1)
        down = shift(down, -1)
        arrived += [up, down]
    arrived.append(shift(up if last == 1 else down, last))
    return arrived


def cross(chosen):
    got = [chosen[0]]
    for step in range(1, NX):
        got.append(lax.ppermute(chosen[step], "leaf", across(step)))
    return got


def flip(value):
    return lax.ppermute(value, "leaf", FLIP)


def exchange(chosen):
    return lax.all_to_all(
        chosen, "leaf", split_axis=0, concat_axis=0, axis_index_groups=ROW_GROUPS, tiled=True
    )


def join_planes(quarter):
    joined = []
    for step in (1, NY - 1, 2):
        joined.append(lax.ppermute(quarter, "rhs", [(i, (i + step) % NY) for i in range(NY)]))
    return joined


def on_device(coords, rhs, basis, transfer_one, transfer_two, far_blocks, neighbours, far_lists):
    me = lax.axis_index("leaf").astype(jnp.int32)
    y = lax.axis_index("rhs").astype(jnp.int32).reshape(1)
    c, z, x = me % NC, (me // NC) % NZ, me // (NC * NZ)
    group = x * NC + c
    payload = pack(y, rhs, coords)
    other_coords = flip(coords)
    leaves = travel(payload, 1)
    nodes = travel(skeletons(payload, basis, transfer_one, transfer_two), -1)
    send_leaf, send_node, take_leaf, take_node = tables(neighbours, far_lists, x, z, c, group)
    targets, self_part = own_tiles(y, rhs, coords, other_coords)
    near = ()
    for chunks in LEAF_CHUNKS:
        got = []
        for low, high in chunks:
            got += cross(choose(low, send_leaf, leaves[low:high], "leaf"))
        quarter = quarters(got)
        pieces = [quarter] + join_planes(quarter)
        near = near_chunk(chunks, take_leaf, got, pieces, targets, near)
    own, other = near
    other = flip(other)
    got = exchange(choose(0, send_node, nodes, "node"))
    far = far_part(take_node, got, far_blocks.reshape(NODE_DEV * FAR, RANK, RANK))
    return finish(far, transfer_one, transfer_two, basis, self_part, own, other)


def solution(mesh):
    return jax.shard_map(
        on_device,
        mesh=mesh,
        in_specs=(
            P(None, "leaf"),
            P("rhs", "leaf"),
            P("leaf", None, None),
            P("leaf", None, None),
            P("leaf", None, None),
            P("leaf", None, None, None),
            P(),
            P(),
        ),
        out_specs=P("rhs", "leaf"),
        check_vma=False,
    )
```
